32 devices in a mesh: groups: 2 (over x), tensor: 16 (over z, y, core).
Axes of the slice: x: 2, y: 2, z: 4, core: 2. Of those that a mesh axis runs over, the one named last changes fastest.
Arguments:
- stem_field: float32 [8, 2, 262144], P('groups', None, 'tensor'), parts along dimension 0, may hold values from -6 to 6
- branches: float32 [4, 2, 2, 256, 256], P(None, None, None, None, 'tensor'), may hold values from -0.25 to 0.25
- branch_order: int32 [4], replicated, may hold values from 0 to 3, each once
- slice_values: int32 [8, 4], P('groups'), parts along dimension 0, may hold values from 0 to 1
Outputs:
- amplitudes: float32 [4, 262144], P('groups', 'tensor'), parts along dimension 0
The draws below stay inside these ranges and needn't reach their ends.
There are 2 independent parts, one for each index of `groups`. The reference program is written for one: setup_inputs(seed, part) draws one part's arguments, and reference() takes and returns one part's arrays. A program takes and returns all parts, laid end to end along the dimension named above; an argument that names none is the same for every part. Nothing has to cross between parts.
Inputs may be any that keep to these rules, and one draw needn't show every extreme that they name: `branch_order`: each branch is merged exactly once.
All inputs are finite; a program needn't handle non-finite values.
Results may differ from the reference program's by a relative error of at most 0.00014.
Values sent between devices are 32-bit elements; how exact they have to be, the bound alone decides.
A program may use at most 64 MiB of HBM per device.

```python
import jax
import jax.numpy as jnp
from jax import lax

S = 4
STEPS = 4
CB = 256
Q_DEV = 16384
NQ = 262144
N_TENSOR = 16


def plant(array, stream_key, low, top_value):
    shape = array.shape
    spot = [jax.random.randint(jax.random.fold_in(stream_key, axis), (), 0, shape[axis]) for axis in range(len(shape))]
    array = array.at[tuple(spot)].set(low)
    longest = shape.index(max(shape))
    spot[longest] = (spot[longest] + 1) % shape[longest]
    return array.at[tuple(spot)].set(top_value)


def steps_of(key, dims, split, smallest, largest):
    gain, own = 1.0, jax.random.fold_in(key, 6)
    for position, parts in split:
        heights = jnp.exp(jax.random.uniform(jax.random.fold_in(own, position), (parts,), jnp.float32, smallest / len(split), largest / len(split)))
        gain = gain * jnp.repeat(heights, dims[position] // parts).reshape([-1 if axis == position else 1 for axis in range(len(dims))])
    return gain


def centred(rng, dims, scale, limit, cuts=(), held_as=jnp.bfloat16):
    drawn = jax.random.normal(rng, dims, jnp.float32) * scale
    if len(cuts) > 0:
        drawn = steps_of(rng, dims, cuts, -0.22, 0.18) * drawn
    return jnp.clip(drawn, min=-limit, max=limit).astype(held_as)


def setup_inputs(seed: int = 0, part: int = 0) -> dict:
    key_of = jax.random.split(jax.random.key(seed), 5)
    part_splits = jax.random.split(jax.random.fold_in(key_of[4], part), 5)
    stem_field = centred(part_splits[0], (S, 2, NQ), 1.0, 6.0, ((2, 16),), jnp.float32)
    branches = centred(key_of[1], (STEPS, 2, 2, CB, CB), (2 * CB) ** -0.5, 0.25, ((4, 16),), jnp.float32)
    branch_order = jax.random.permutation(key_of[2], STEPS).astype(jnp.int32)
    slice_values = plant(jax.random.randint(part_splits[3], (S, STEPS), 0, 2), jax.random.fold_in(part_splits[3], 1), 0, 1).astype(jnp.int32)
    return {"stem_field": stem_field, "branches": branches, "branch_order": branch_order, "slice_values": slice_values}


def product(left, right):
    return jnp.einsum('shmi,sil->shml', left, right, precision=lax.Precision.HIGHEST)


def reference(stem_field, branches, branch_order, slice_values):
    shards = N_TENSOR
    middle = Q_DEV // CB
    current = stem_field
    for step_index in range(STEPS):
        branch_now = branches[branch_order[step_index]]
        values_now = slice_values[:, step_index]
        chosen = jnp.where((values_now == 1)[:, None, None, None], branch_now[1][None], branch_now[0][None])
        blocks = current.reshape(S, 2, shards, middle, CB)
        real_part = product(blocks[:, 0], chosen[:, 0]) - product(blocks[:, 1], chosen[:, 1])
        imag_part = product(blocks[:, 0], chosen[:, 1]) + product(blocks[:, 1], chosen[:, 0])
        combined = jnp.stack([real_part, imag_part], axis=1)
        combined = combined.reshape(S, 2, shards, middle, shards, CB // shards)
        current = combined.transpose(0, 1, 4, 2, 5, 3).reshape(S, 2, shards * Q_DEV)
    return jnp.sum(current, axis=0)
```

```python
import functools

import jax
import jax.numpy as jnp
from jax import lax
from jax.experimental import pallas as pl
from jax.experimental.pallas import tpu as pltpu
from jax.sharding import PartitionSpec as P

MESH = pl.DeviceIdType.MESH


def product(left, right):
    return jnp.einsum("smi,sil->slm", left, right, precision=lax.Precision.HIGHEST)


def combine_branch(stem_part, branch_now, values_now):
    slices, _, _, width = stem_part.shape
    chosen = jnp.where(
        (values_now == 1)[:, None, None, None], branch_now[1][None], branch_now[0][None]
    )
    real_part = product(stem_part[:, 0], chosen[:, 0]) - product(stem_part[:, 1], chosen[:, 1])
    imag_part = product(stem_part[:, 0], chosen[:, 1]) + product(stem_part[:, 1], chosen[:, 0])
    return jnp.stack([real_part, imag_part], axis=1)


def plain_device(stem_field, branches, branch_order, slice_values):
    shards = lax.axis_size("tensor")
    steps = branches.shape[0]
    width = branches.shape[3]
    current = stem_field
    for step in range(steps):
        table = lax.all_gather(
            lax.dynamic_index_in_dim(branches, branch_order[step], 0, keepdims=False),
            "tensor",
            axis=3,
            tiled=True,
        )
        slices, parts, entries = current.shape
        blocks = current.reshape(slices, parts, entries // width, width)
        combined = combine_branch(blocks, table, slice_values[:, step])
        combined = combined.reshape(slices, parts, shards, width // shards, entries // width)
        current = lax.all_to_all(
            combined, "tensor", split_axis=2, concat_axis=2, tiled=True
        ).reshape(current.shape)
    return jnp.sum(current, axis=0)


def split(value):
    high = value.astype(jnp.bfloat16)
    return high, (value - high.astype(jnp.float32)).astype(jnp.bfloat16)


def kernel(cfg, values, stem, shard, out, g0, g1, g2, g3, w, y, sent, got, fsent,
           ring_sem, pair_sem, side_sem, cross_sem, send_sem, x_sem, f_sem, xs_sem, fs_sem):
    T, S, K, CB, M, CLO, CHI = cfg
    chips = T // 2
    zs = chips // 2
    gs = (g0, g1, g2, g3)
    gx = lax.axis_index("groups")
    me = lax.axis_index("tensor")
    core = lax.rem(me, 2)
    col = lax.rem(me // 2, 2)
    depth = me // 4
    pos = jnp.where(col == 0, depth, chips - 1 - depth)

    def at(position, which):
        p = lax.rem(position + 2 * chips, chips)
        z = jnp.where(p < zs, p, chips - 1 - p)
        c = jnp.where(p < zs, 0, 1)
        return (z * 2 + c) * 2 + which

    right, left = at(pos + 1, core), at(pos - 1, core)
    partner = me + 1 - 2 * core

    barrier = pltpu.get_barrier_semaphore()
    for d in range(1, T):
        pl.semaphore_signal(barrier, inc=1, device_id=(gx, lax.rem(me + d, T)), device_id_type=MESH)
    pl.semaphore_signal(barrier, inc=1, device_id=(1 - gx, me), device_id_type=MESH)
    pl.semaphore_wait(barrier, T)

    started = []

    def push(src, dst, ssem, rsem, device):
        copy = pltpu.make_async_remote_copy(
            src_ref=src, dst_ref=dst, send_sem=ssem, recv_sem=rsem,
            device_id=device, device_id_type=MESH,
        )
        copy.start()
        return copy

    counter = [0] * 4
    own_part = pl.ds(gx, 3)

    def hop(t, rel, to, device):
        n = counter[t]
        counter[t] += 1
        src = (shard.at[t] if rel == 0 else gs[t].at[0, rel]).at[own_part]
        started.append(push(src, gs[t].at[0, to].at[own_part], send_sem.at[t, n],
                            ring_sem.at[t, to], (gx, device)))

    def pair(t, rel):
        n = counter[t]
        counter[t] += 1
        if rel == 0:
            src, dst = shard.at[t], gs[t].at[1, 0]
        else:
            src, dst = gs[t].at[0, rel].at[own_part], gs[t].at[1, rel].at[own_part]
        started.append(push(src, dst, send_sem.at[t, n], pair_sem.at[t, rel], (gx, partner)))

    def await_ring(t, rel):
        dst = gs[t].at[0, rel].at[own_part]
        pltpu.make_async_remote_copy(
            src_ref=dst, dst_ref=dst, send_sem=ring_sem.at[t, rel], recv_sem=ring_sem.at[t, rel],
            device_id=(gx, right), device_id_type=MESH).wait_recv()

    def begin(t):
        hop(t, 0, chips - 1, right)
        hop(t, 0, 1, left)
        pair(t, 0)

    def advance(t, k):
        half = chips // 2
        if k < half:
            rel = chips - k
            await_ring(t, rel)
            if k < half - 1 or t % 2 == 0:
                hop(t, rel, rel - 1, right)
            pair(t, rel)
            await_ring(t, k)
            if k < half - 1 or t % 2 == 1:
                hop(t, k, k + 1, left)
            pair(t, k)
        else:
            await_ring(t, half)
            pair(t, half)
            n = counter[t]
            counter[t] += 1
            lane = gs[t].at[0, pl.ds(1, chips - 1), gx * 3]
            started.append(push(lane, lane, send_sem.at[t, n], side_sem.at[t], (1 - gx, me)))

    def finish(t):
        lane = gs[t].at[0, pl.ds(1, chips - 1), (1 - gx) * 3]
        pltpu.make_async_remote_copy(
            src_ref=lane, dst_ref=lane, send_sem=side_sem.at[t], recv_sem=side_sem.at[t],
            device_id=(1 - gx, me), device_id_type=MESH).wait_recv()
        n = counter[t]
        counter[t] += 1
        there = gs[t].at[1, pl.ds(1, chips - 1), (1 - gx) * 3]
        started.append(push(lane, there, send_sem.at[t, n], cross_sem.at[t], (gx, partner)))

    def settle(t):
        for rel in range(chips):
            dst = gs[t].at[1, 0] if rel == 0 else gs[t].at[1, rel].at[own_part]
            pltpu.make_async_remote_copy(
                src_ref=dst, dst_ref=dst, send_sem=pair_sem.at[t, rel], recv_sem=pair_sem.at[t, rel],
                device_id=(gx, partner), device_id_type=MESH).wait_recv()
        there = gs[t].at[1, pl.ds(1, chips - 1), (1 - gx) * 3]
        pltpu.make_async_remote_copy(
            src_ref=there, dst_ref=there, send_sem=cross_sem.at[t], recv_sem=cross_sem.at[t],
            device_id=(gx, partner), device_id_type=MESH).wait_recv()

    def load_tables(t):
        g = gs[t]
        for a in range(T):
            z, c, which = a // 4, (a // 2) % 2, a % 2
            apos = z if c == 0 else chips - 1 - z
            rel = lax.rem(apos - pos + chips, chips)
            other = jnp.where(core == which, 0, 1)
            mine = jnp.logical_and(rel == 0, other == 0)
            for v in range(2):
                for p in range(2):
                    block = jnp.where(mine, shard[t, 2 * v + p], g[other, rel, 2 * v + p])
                    high, low = split(block)
                    rows = slice(a * K, (a + 1) * K)
                    cols = slice(p * CB, (p + 1) * CB)
                    w[v, 0, rows, cols] = high
                    w[v, 1, rows, cols] = low

    def merge(v, real, imag):
        rh, rl = split(real)
        ih, il = split(imag)
        ah = jnp.concatenate([jnp.concatenate([rh, -ih], axis=1), jnp.concatenate([ih, rh], axis=1)], axis=0)
        al = jnp.concatenate([jnp.concatenate([rl, -il], axis=1), jnp.concatenate([il, rl], axis=1)], axis=0)
        dims = (((1,), (1,)), ((), ()))
        dot = functools.partial(lax.dot_general, dimension_numbers=dims,
                                preferred_element_type=jnp.float32)
        wh, wl = w[v, 0], w[v, 1]
        return dot(wh, ah) + (dot(wh, al) + dot(wl, ah))

    def regroup(ref, chi_major):
        rows = CB // CLO
        pieces = []
        for lo in range(CLO):
            if chi_major:
                pieces.append(jnp.concatenate(
                    [ref[pl.ds(c * CLO + lo, T, stride=K), :] for c in range(CHI)], axis=0))
            else:
                pieces.append(ref[pl.ds(lo, rows, stride=CLO), :])
        return [jnp.concatenate([b[:, p * M:(p + 1) * M] for b in pieces], axis=1) for p in range(2)]

    for t in range(4):
        begin(t)
    for k in range(1, chips // 2 + 1):
        for t in range(4):
            advance(t, k)
    for t in range(4):
        finish(t)

    settle(0)
    load_tables(0)
    for s in range(S):
        y[s] = merge(values[s, 0], stem[s, 0], stem[s, 1])
    settle(1)
    load_tables(1)
    for s in range(S):
        real, imag = regroup(y.at[s], True)
        r = merge(values[s, 1], real, imag)
        for a in range(T):
            sent[pl.ds((a * S + s) * K, K), :] = r[a * K:(a + 1) * K]
    span = S * K
    block_of = lambda i: pl.ds(pl.multiple_of(i * span, span), span)
    copies = []
    for d in range(1, T):
        to = lax.rem(me + d, T)
        copies.append(push(sent.at[block_of(to)], got.at[block_of(me)], xs_sem.at[d], x_sem.at[d], (gx, to)))
    got[block_of(me), :] = sent[block_of(me), :]
    settle(2)
    load_tables(2)
    for d in range(1, T):
        frm = lax.rem(me - d + T, T)
        dst = got.at[block_of(frm)]
        pltpu.make_async_remote_copy(
            src_ref=dst, dst_ref=dst, send_sem=x_sem.at[d], recv_sem=x_sem.at[d],
            device_id=(gx, frm), device_id_type=MESH).wait_recv()
    sums = [None, None]
    for s in range(S):
        parts = [[], []]
        for hi in range(CHI):
            block = jnp.concatenate(
                [got[pl.ds(s * K + hi * CLO + lo, T, stride=span), :] for lo in range(CLO)], axis=0)
            turned = block.T
            for p in range(2):
                parts[p].append(jnp.concatenate(
                    [turned[(p * CHI + c) * T:(p * CHI + c + 1) * T] for c in range(CHI)], axis=1))
        real, imag = [jnp.concatenate(q, axis=0) for q in parts]
        r = merge(values[s, 2], real, imag)
        one = values[s, 3] == 1
        for v in range(2):
            part = jnp.where(one if v else jnp.logical_not(one), r, 0.0)
            sums[v] = part if s == 0 else sums[v] + part
    y[0] = sums[0]
    y[1] = sums[1]
    settle(3)
    load_tables(3)
    total = None
    for v in range(2):
        real, imag = regroup(y.at[v], False)
        r = merge(v, real, imag)
        total = r if v == 0 else total + r
    fsent[...] = total
    row_of = lambda i: pl.ds(pl.multiple_of(i * K, K), K)
    for d in range(1, T):
        to = lax.rem(me + d, T)
        copies.append(push(fsent.at[row_of(to)], out.at[row_of(me)], fs_sem.at[d], f_sem.at[d], (gx, to)))
    out[row_of(me), :] = fsent[row_of(me), :]
    for d in range(1, T):
        frm = lax.rem(me - d + T, T)
        dst = out.at[row_of(frm)]
        pltpu.make_async_remote_copy(
            src_ref=dst, dst_ref=dst, send_sem=f_sem.at[d], recv_sem=f_sem.at[d],
            device_id=(gx, frm), device_id_type=MESH).wait_recv()
    for copy in started + copies:
        copy.wait_send()


def fused_device(stem_field, branches, branch_order, slice_values):
    T = lax.axis_size("tensor")
    S, _, entries = stem_field.shape
    steps, _, _, CB, K = branches.shape
    M = entries // CB
    CLO = CB // M
    CHI = K // CLO
    stem = stem_field.reshape(S, 2, M, CB)
    shard = jnp.take(branches, branch_order, axis=0).reshape(steps, 4, CB, K).transpose(0, 1, 3, 2)
    third = shard[2].reshape(4, K, CLO, T, CHI).transpose(0, 1, 4, 2, 3).reshape(4, K, CB)
    fourth = shard[3].reshape(4, K, CLO, T, CHI).transpose(0, 1, 2, 4, 3).reshape(4, K, CB)
    shard = jnp.stack([shard[0], shard[1], third, fourth])
    vmem = pl.BlockSpec(memory_space=pltpu.VMEM)
    dma = pltpu.SemaphoreType.DMA
    table = pltpu.VMEM((2, T // 2, 4, K, CB), jnp.float32)
    moved = pltpu.VMEM((T * S * K, 2 * M), jnp.float32)
    gathered = pl.pallas_call(
        functools.partial(kernel, (T, S, K, CB, M, CLO, CHI)),
        out_shape=jax.ShapeDtypeStruct((T * K, 2 * M), jnp.float32),
        in_specs=[pl.BlockSpec(memory_space=pltpu.SMEM), vmem, vmem],
        out_specs=vmem,
        scratch_shapes=[
            table, table, table, table,
            pltpu.VMEM((2, 2, CB, 2 * CB), jnp.bfloat16),
            pltpu.VMEM((S, CB, 2 * M), jnp.float32),
            moved, moved,
            pltpu.VMEM((CB, 2 * M), jnp.float32),
            dma((4, T // 2)), dma((4, T // 2)), dma((4,)), dma((4,)),
            dma((4, 20)),
            dma((T,)), dma((T,)), dma((T,)), dma((T,)),
        ],
        compiler_params=pltpu.CompilerParams(collective_id=0, has_side_effects=True),
    )(slice_values, stem, shard)
    ordered = gathered.reshape(T, K, 2, T, CHI).transpose(2, 3, 1, 0, 4)
    return ordered.reshape(2, entries)


def solution(mesh):
    def per_device(stem_field, branches, branch_order, slice_values):
        shards = lax.axis_size("tensor")
        steps, _, _, width, columns = branches.shape
        middle = stem_field.shape[2] // width
        fits = (
            mesh.shape["groups"] == 2 and shards % 8 == 0 and columns % 8 == 0 and steps == 4
            and 2 * middle == 128 and width % middle == 0 and columns % (width // middle) == 0
        )
        run = fused_device if fits else plain_device
        return run(stem_field, branches, branch_order, slice_values)

    return jax.shard_map(
        per_device,
        mesh=mesh,
        in_specs=(
            P("groups", None, "tensor"),
            P(None, None, None, None, "tensor"),
            P(),
            P("groups", None),
        ),
        out_specs=P("groups", "tensor"),
        check_vma=False,
    )
```

```python
import functools

import jax
import jax.numpy as jnp
from jax import lax
from jax.experimental import pallas as pl
from jax.experimental.pallas import tpu as pltpu
from jax.sharding import PartitionSpec as P

MESH = pl.DeviceIdType.MESH


def product(left, right):
    return jnp.einsum("smi,sil->slm", left, right, precision=lax.Precision.HIGHEST)


def combine_branch(stem_part, branch_now, values_now):
    slices, _, _, width = stem_part.shape
    chosen = jnp.where(
        (values_now == 1)[:, None, None, None], branch_now[1][None], branch_now[0][None]
    )
    real_part = product(stem_part[:, 0], chosen[:, 0]) - product(stem_part[:, 1], chosen[:, 1])
    imag_part = product(stem_part[:, 0], chosen[:, 1]) + product(stem_part[:, 1], chosen[:, 0])
    return jnp.stack([real_part, imag_part], axis=1)


def plain_device(stem_field, branches, branch_order, slice_values):
    shards = lax.axis_size("tensor")
    steps = branches.shape[0]
    width = branches.shape[3]
    current = stem_field
    for step in range(steps):
        table = lax.all_gather(
            lax.dynamic_index_in_dim(branches, branch_order[step], 0, keepdims=False),
            "tensor",
            axis=3,
            tiled=True,
        )
        slices, parts, entries = current.shape
        blocks = current.reshape(slices, parts, entries // width, width)
        combined = combine_branch(blocks, table, slice_values[:, step])
        combined = combined.reshape(slices, parts, shards, width // shards, entries // width)
        current = lax.all_to_all(
            combined, "tensor", split_axis=2, concat_axis=2, tiled=True
        ).reshape(current.shape)
    return jnp.sum(current, axis=0)


def split(value):
    high = value.astype(jnp.bfloat16)
    return high, (value - high.astype(jnp.float32)).astype(jnp.bfloat16)


def kernel(cfg, values, stem, shard, out, g0, g1, g2, g3, w0, w1, w2, w3, y, sent, got, fsent, fgot, turned_f,
           ring_sem, pair_sem, side_sem, cross_sem, send_sem, x_sem, f_sem, xs_sem, fs_sem):
    T, S, K, CB, M, CLO, CHI = cfg
    chips = T // 2
    half = chips // 2
    zs = chips // 2
    gs = (g0, g1, g2, g3)
    ws = (w0, w1, w2, w3)
    gx = lax.axis_index("groups")
    me = lax.axis_index("tensor")
    core = lax.rem(me, 2)
    col = lax.rem(me // 2, 2)
    depth = me // 4
    pos = jnp.where(col == 0, depth, chips - 1 - depth)

    def at(position, which):
        p = lax.rem(position + 2 * chips, chips)
        z = jnp.where(p < zs, p, chips - 1 - p)
        c = jnp.where(p < zs, 0, 1)
        return (z * 2 + c) * 2 + which

    right, left = at(pos + 1, core), at(pos - 1, core)
    partner = me + 1 - 2 * core

    barrier = pltpu.get_barrier_semaphore()
    for d in range(1, T):
        pl.semaphore_signal(barrier, inc=1, device_id=(gx, lax.rem(me + d, T)), device_id_type=MESH)
    pl.semaphore_signal(barrier, inc=1, device_id=(1 - gx, me), device_id_type=MESH)
    pl.semaphore_wait(barrier, T)

    started = []
    counter = [0] * 4
    own_part = pl.ds(gx, 3)
    out_part = gx * 3
    in_part = (1 - gx) * 3

    def push(src, dst, ssem, rsem, device):
        copy = pltpu.make_async_remote_copy(
            src_ref=src, dst_ref=dst, send_sem=ssem, recv_sem=rsem,
            device_id=device, device_id_type=MESH,
        )
        copy.start()
        started.append(copy)

    def arrived(dst, rsem):
        pltpu.make_async_remote_copy(
            src_ref=dst, dst_ref=dst, send_sem=rsem, recv_sem=rsem,
            device_id=(gx, partner), device_id_type=MESH).wait_recv()

    def token(t):
        counter[t] += 1
        return send_sem.at[t, counter[t] - 1]

    def hop(t, rel, to, device):
        src = (shard.at[t] if rel == 0 else gs[t].at[0, rel]).at[own_part]
        push(src, gs[t].at[0, to].at[own_part], token(t), ring_sem.at[t, to], (gx, device))

    def spread(t, rel):
        src = gs[t].at[0, rel]
        push(src.at[out_part], src.at[out_part], token(t), side_sem.at[t, rel], (1 - gx, me))
        push(src.at[own_part], gs[t].at[1, rel].at[own_part], token(t), pair_sem.at[t, rel], (gx, partner))

    def cross(t, rel):
        src = gs[t].at[0, rel].at[in_part]
        arrived(src, side_sem.at[t, rel])
        push(src, gs[t].at[1, rel].at[in_part], token(t), cross_sem.at[t, rel], (gx, partner))

    def begin(t):
        hop(t, 0, chips - 1, right)
        hop(t, 0, 1, left)
        push(shard.at[t], gs[t].at[1, 0], token(t), pair_sem.at[t, 0], (gx, partner))

    def advance(t, k):
        if k < half:
            rel = chips - k
            arrived(gs[t].at[0, rel].at[own_part], ring_sem.at[t, rel])
            if k < half - 1 or t % 2 == 0:
                hop(t, rel, rel - 1, right)
            spread(t, rel)
            arrived(gs[t].at[0, k].at[own_part], ring_sem.at[t, k])
            if k < half - 1 or t % 2 == 1:
                hop(t, k, k + 1, left)
            spread(t, k)
        else:
            arrived(gs[t].at[0, half].at[own_part], ring_sem.at[t, half])
            spread(t, half)
        if k > 1:
            cross(t, chips - k + 1)
            cross(t, k - 1)
        if k == half:
            cross(t, half)

    def settle(t):
        arrived(gs[t].at[1, 0], pair_sem.at[t, 0])
        for rel in range(1, chips):
            arrived(gs[t].at[1, rel].at[own_part], pair_sem.at[t, rel])
            arrived(gs[t].at[1, rel].at[in_part], cross_sem.at[t, rel])

    def load_tables(t):
        settle(t)
        g, w = gs[t], ws[t]
        for a in range(T):
            z, c, which = a // 4, (a // 2) % 2, a % 2
            apos = z if c == 0 else chips - 1 - z
            rel = lax.rem(apos - pos + chips, chips)
            other = jnp.where(core == which, 0, 1)
            for v in range(2):
                for p in range(2):
                    high, low = split(g[other, rel, 2 * v + p])
                    rows = slice(a * K, (a + 1) * K)
                    cols = slice(p * CB, (p + 1) * CB)
                    w[v, 0, rows, cols] = high
                    w[v, 1, rows, cols] = low
        if t >= 2 and CHI > 1:
            row = lax.broadcasted_iota(jnp.int32, (CB, CB), 0)
            lane = lax.broadcasted_iota(jnp.int32, (CB, CB), 1)
            if t == 2:
                c, lo, h = lane // (CLO * T), (lane // T) % CLO, lane % T
            else:
                lo, c, h = lane // (CHI * T), (lane // T) % CHI, lane % T
            move = (row == (lo * T + h) * CHI + c).astype(jnp.float32).astype(jnp.bfloat16)
            for v in range(2):
                for i in range(2):
                    for p in range(2):
                        cols = slice(p * CB, (p + 1) * CB)
                        w[v, i, :, cols] = jnp.dot(
                            w[v, i, :, cols], move, preferred_element_type=jnp.float32
                        ).astype(jnp.bfloat16)

    def merge(t, v, real, imag):
        rh, rl = split(real)
        ih, il = split(imag)
        ah = jnp.concatenate([jnp.concatenate([rh, -ih], axis=1), jnp.concatenate([ih, rh], axis=1)], axis=0)
        al = jnp.concatenate([jnp.concatenate([rl, -il], axis=1), jnp.concatenate([il, rl], axis=1)], axis=0)
        dims = (((1,), (1,)), ((), ()))
        dot = functools.partial(lax.dot_general, dimension_numbers=dims,
                                preferred_element_type=jnp.float32)
        wh, wl = ws[t][v, 0], ws[t][v, 1]
        return dot(wh, ah) + (dot(wh, al) + dot(wl, ah))

    def regroup(ref, chi_major):
        rows = CB // CLO
        pieces = []
        for lo in range(CLO):
            if chi_major:
                pieces.append(jnp.concatenate(
                    [ref[pl.ds(c * CLO + lo, T, stride=K), :] for c in range(CHI)], axis=0))
            else:
                pieces.append(ref[pl.ds(lo, rows, stride=CLO), :])
        return [jnp.concatenate([b[:, p * M:(p + 1) * M] for b in pieces], axis=1) for p in range(2)]

    order = sorted(((t, k) for t in range(4) for k in range(half + 1)), key=lambda i: (i[1] + 1.1 * i[0], i[0]))
    pending = []
    for item in order:
        if item[1] == 0:
            begin(item[0])
        elif item == (0, half):
            advance(*item)
            break
        else:
            advance(*item)
    pending = list(order[order.index((0, half)) + 1:])

    def more(count=1):
        for _ in range(count):
            if pending:
                t, k = pending.pop(0)
                if k == 0:
                    begin(t)
                else:
                    advance(t, k)

    for t in range(4):
        gs[t][0, 0] = shard[t]
    load_tables(0)
    for s in range(S):
        y[s] = merge(0, values[s, 0], stem[s, 0], stem[s, 1])
        more()
    while any(t == 1 for t, k in pending):
        more()
    load_tables(1)
    rows_of = lambda s, i: pl.ds(pl.multiple_of((s * T + i) * K, K), K)
    for s in range(S):
        real, imag = regroup(y.at[s], True)
        sent[pl.ds(s * T * K, T * K), :] = merge(1, values[s, 1], real, imag)
        for d in range(1, T):
            to = lax.rem(me + d, T)
            push(sent.at[rows_of(s, to)], got.at[rows_of(s, me)], xs_sem.at[s, d], x_sem.at[s, d], (gx, to))
        got[rows_of(s, me), :] = sent[rows_of(s, me), :]
        more()
    more(len(pending))
    load_tables(2)
    load_tables(3)
    sums = [None, None]
    for s in range(S):
        for d in range(1, T):
            frm = lax.rem(me - d + T, T)
            arrived(got.at[rows_of(s, frm)], x_sem.at[s, d])
        parts = [[], []]
        for hi in range(CHI):
            block = jnp.concatenate(
                [got[pl.ds(s * T * K + hi * CLO + lo, T, stride=K), :] for lo in range(CLO)], axis=0)
            turned = block.T
            for p in range(2):
                parts[p].append(jnp.concatenate(
                    [turned[(p * CHI + c) * T:(p * CHI + c + 1) * T] for c in range(CHI)], axis=1))
        real, imag = [jnp.concatenate(q, axis=0) for q in parts]
        r = merge(2, values[s, 2], real, imag)
        one = values[s, 3] == 1
        for v in range(2):
            part = jnp.where(one if v else jnp.logical_not(one), r, 0.0)
            sums[v] = part if s == 0 else sums[v] + part
    y[0] = sums[0]
    y[1] = sums[1]
    total = None
    for v in range(2):
        real, imag = regroup(y.at[v], False)
        r = merge(3, v, real, imag)
        total = r if v == 0 else total + r
    fsent[...] = total
    row_of = lambda i: pl.ds(pl.multiple_of(i * K, K), K)
    for d in range(1, T):
        to = lax.rem(me + d, T)
        push(fsent.at[row_of(to)], fgot.at[row_of(me)], fs_sem.at[d], f_sem.at[d], (gx, to))
    fgot[row_of(me), :] = fsent[row_of(me), :]
    for d in range(1, T):
        frm = lax.rem(me - d + T, T)
        arrived(fgot.at[row_of(frm)], f_sem.at[d])

    lanes = 2 * M
    width = lanes // CHI
    across = jnp.concatenate([fgot[pl.ds(c, T, stride=K), :] for c in range(K)], axis=0)
    halves = CB // lanes
    for i in range(halves):
        turned_f[i] = across[i * lanes:(i + 1) * lanes].T
    pieces = [jnp.concatenate(
        [turned_f[i, pl.ds(c, 2 * T, stride=CHI), :] for i in range(halves)], axis=1) for c in range(CHI)]
    count = CB // width
    lined = jnp.concatenate(
        [jnp.concatenate([q[:, j * width:(j + 1) * width] for q in pieces], axis=1) for j in range(count)], axis=0)
    row = lax.broadcasted_iota(jnp.int32, (lanes, lanes), 0)
    lane = lax.broadcasted_iota(jnp.int32, (lanes, lanes), 1)
    move = (row == (lane % CHI) * width + lane // CHI).astype(jnp.float32).astype(jnp.bfloat16)
    first, rest = lined.astype(jnp.bfloat16), lined
    rest = rest - first.astype(jnp.float32)
    second, third = split(rest)
    dot = functools.partial(jnp.dot, preferred_element_type=jnp.float32)
    placed = (dot(first, move) + dot(second, move)) + dot(third, move)
    for j in range(count):
        out[:, j * lanes:(j + 1) * lanes] = placed[j * 2 * T:(j + 1) * 2 * T]
    for copy in started:
        copy.wait_send()


def fused_device(stem_field, branches, branch_order, slice_values):
    T = lax.axis_size("tensor")
    S, _, entries = stem_field.shape
    steps, _, _, CB, K = branches.shape
    M = entries // CB
    CLO = CB // M
    CHI = K // CLO
    stem = stem_field.reshape(S, 2, M, CB)
    shard = jnp.take(branches, branch_order, axis=0).reshape(steps, 4, CB, K).transpose(0, 1, 3, 2)
    vmem = pl.BlockSpec(memory_space=pltpu.VMEM)
    dma = pltpu.SemaphoreType.DMA
    table = pltpu.VMEM((2, T // 2, 4, K, CB), jnp.float32)
    merged = pltpu.VMEM((2, 2, CB, 2 * CB), jnp.bfloat16)
    moved = pltpu.VMEM((T * S * K, 2 * M), jnp.float32)
    gathered = pl.pallas_call(
        functools.partial(kernel, (T, S, K, CB, M, CLO, CHI)),
        out_shape=jax.ShapeDtypeStruct((2 * T, entries // T), jnp.float32),
        in_specs=[pl.BlockSpec(memory_space=pltpu.SMEM), vmem, vmem],
        out_specs=vmem,
        scratch_shapes=[
            table, table, table, table,
            merged, merged, merged, merged,
            pltpu.VMEM((S, CB, 2 * M), jnp.float32),
            moved, moved,
            pltpu.VMEM((CB, 2 * M), jnp.float32),
            pltpu.VMEM((CB, 2 * M), jnp.float32),
            pltpu.VMEM((CB // (2 * M), 2 * M, 2 * M), jnp.float32),
            dma((4, T // 2)), dma((4, T // 2)), dma((4, T // 2)), dma((4, T // 2)),
            dma((4, 2 * T + 2)),
            dma((S, T)), dma((T,)), dma((S, T)), dma((T,)),
        ],
        compiler_params=pltpu.CompilerParams(collective_id=0, has_side_effects=True),
    )(slice_values, stem, shard)
    return gathered.reshape(2, entries)


def solution(mesh):
    def per_device(stem_field, branches, branch_order, slice_values):
        shards = lax.axis_size("tensor")
        steps, _, _, width, columns = branches.shape
        middle = stem_field.shape[2] // width
        fits = (
            mesh.shape["groups"] == 2 and shards % 8 == 0 and columns % 8 == 0 and steps == 4
            and 2 * middle == 128 and width % middle == 0 and columns % (width // middle) == 0
        )
        run = fused_device if fits else plain_device
        return run(stem_field, branches, branch_order, slice_values)

    return jax.shard_map(
        per_device,
        mesh=mesh,
        in_specs=(
            P("groups", None, "tensor"),
            P(None, None, None, None, "tensor"),
            P(),
            P("groups", None),
        ),
        out_specs=P("groups", "tensor"),
        check_vma=False,
    )
```

```python
import functools

import jax
import jax.numpy as jnp
from jax import lax
from jax.experimental import pallas as pl
from jax.experimental.pallas import tpu as pltpu
from jax.sharding import PartitionSpec as P

MESH = pl.DeviceIdType.MESH


def product(left, right):
    return jnp.einsum("smi,sil->slm", left, right, precision=lax.Precision.HIGHEST)


def combine_branch(stem_part, branch_now, values_now):
    slices, _, _, width = stem_part.shape
    chosen = jnp.where(
        (values_now == 1)[:, None, None, None], branch_now[1][None], branch_now[0][None]
    )
    real_part = product(stem_part[:, 0], chosen[:, 0]) - product(stem_part[:, 1], chosen[:, 1])
    imag_part = product(stem_part[:, 0], chosen[:, 1]) + product(stem_part[:, 1], chosen[:, 0])
    return jnp.stack([real_part, imag_part], axis=1)


def plain_device(stem_field, branches, branch_order, slice_values):
    shards = lax.axis_size("tensor")
    steps = branches.shape[0]
    width = branches.shape[3]
    current = stem_field
    for step in range(steps):
        table = lax.all_gather(
            lax.dynamic_index_in_dim(branches, branch_order[step], 0, keepdims=False),
            "tensor",
            axis=3,
            tiled=True,
        )
        slices, parts, entries = current.shape
        blocks = current.reshape(slices, parts, entries // width, width)
        combined = combine_branch(blocks, table, slice_values[:, step])
        combined = combined.reshape(slices, parts, shards, width // shards, entries // width)
        current = lax.all_to_all(
            combined, "tensor", split_axis=2, concat_axis=2, tiled=True
        ).reshape(current.shape)
    return jnp.sum(current, axis=0)


def split(value):
    high = value.astype(jnp.bfloat16)
    return high, (value - high.astype(jnp.float32)).astype(jnp.bfloat16)


def kernel(cfg, values, stem, shard, out, g0, g1, g2, g3, w0, w1, w2, w3, y, sent, got, fsent, fgot, turned_f,
           gather_sem, send_sem, x_sem, f_sem, xs_sem, fs_sem):
    T, S, K, CB, M, CLO, CHI = cfg
    Z = T // 4
    gs = (g0, g1, g2, g3)
    ws = (w0, w1, w2, w3)
    gx = lax.axis_index("groups")
    me = lax.axis_index("tensor")
    core = lax.rem(me, 2)
    col = lax.rem(me // 2, 2)
    depth = me // 4
    partner = me + 1 - 2 * core
    across_y = me + 2 - 4 * col

    barrier = pltpu.get_barrier_semaphore()
    for d in range(1, T):
        pl.semaphore_signal(barrier, inc=1, device_id=(gx, lax.rem(me + d, T)), device_id_type=MESH)
    pl.semaphore_signal(barrier, inc=1, device_id=(1 - gx, me), device_id_type=MESH)
    pl.semaphore_wait(barrier, T)

    started = []
    counter = [0] * 4
    ours = pl.ds(2 * gx, 2)
    theirs = pl.ds(2 - 2 * gx, 2)
    far = pl.ds(1, Z - 1)

    def push(src, dst, ssem, rsem, device):
        copy = pltpu.make_async_remote_copy(
            src_ref=src, dst_ref=dst, send_sem=ssem, recv_sem=rsem,
            device_id=device, device_id_type=MESH,
        )
        copy.start()
        started.append(copy)

    def arrived(dst, rsem):
        pltpu.make_async_remote_copy(
            src_ref=dst, dst_ref=dst, send_sem=rsem, recv_sem=rsem,
            device_id=(gx, partner), device_id_type=MESH).wait_recv()

    def token(t):
        counter[t] += 1
        return send_sem.at[t, counter[t] - 1]

    def send(t, src, dst, slot, device):
        push(src, dst, token(t), gather_sem.at[t, slot], device)

    def pair(t, row, levels, part, slot):
        send(t, gs[t].at[0, row, levels, part], gs[t].at[1, row, levels, part], slot, (gx, partner))

    def side(t, row, slot):
        src = gs[t].at[0, row, far, ours]
        send(t, src, src, slot, (1 - gx, me))

    def launch(t):
        for d in range(1, Z):
            to = lax.rem(depth + d, Z) * 4 + lax.rem(me, 4)
            send(t, shard.at[t, ours], gs[t].at[0, 0, Z - d, ours], 11 + Z - d, (gx, to))

    def lead(t):
        send(t, shard.at[t], gs[t].at[0, 1, 0], 0, (gx, across_y))
        send(t, shard.at[t], gs[t].at[1, 0, 0], 5, (gx, partner))

    def first(t):
        for d in range(1, Z):
            arrived(gs[t].at[0, 0, d, ours], gather_sem.at[t, 11 + d])
        send(t, gs[t].at[0, 0, far, ours], gs[t].at[0, 1, far, ours], 1, (gx, across_y))
        side(t, 0, 2)
        pair(t, 0, far, ours, 6)
        if t < 3:
            lead(t + 1)

    def second(t):
        arrived(gs[t].at[0, 1, far, ours], gather_sem.at[t, 1])
        side(t, 1, 3)
        pair(t, 1, far, ours, 7)
        arrived(gs[t].at[0, 1, 0], gather_sem.at[t, 0])
        send(t, gs[t].at[0, 1, 0], gs[t].at[1, 1, 0], 8, (gx, partner))

    def third(t):
        arrived(gs[t].at[0, 0, far, theirs], gather_sem.at[t, 2])
        pair(t, 0, far, theirs, 9)
        arrived(gs[t].at[0, 1, far, theirs], gather_sem.at[t, 3])
        pair(t, 1, far, theirs, 10)

    def settle(t):
        arrived(gs[t].at[1, 0, 0], gather_sem.at[t, 5])
        arrived(gs[t].at[1, 0, far, ours], gather_sem.at[t, 6])
        arrived(gs[t].at[1, 1, far, ours], gather_sem.at[t, 7])
        arrived(gs[t].at[1, 1, 0], gather_sem.at[t, 8])
        arrived(gs[t].at[1, 0, far, theirs], gather_sem.at[t, 9])
        arrived(gs[t].at[1, 1, far, theirs], gather_sem.at[t, 10])

    def load_tables(t):
        settle(t)
        g, w = gs[t], ws[t]
        for a in range(T):
            z, c, which = a // 4, (a // 2) % 2, a % 2
            rel = lax.rem(z - depth + Z, Z)
            row = jnp.where(col == c, 0, 1)
            other = jnp.where(core == which, 0, 1)
            for v in range(2):
                for p in range(2):
                    high, low = split(g[other, row, rel, 2 * v + p])
                    rows = slice(a * K, (a + 1) * K)
                    cols = slice(p * CB, (p + 1) * CB)
                    w[v, 0, rows, cols] = high
                    w[v, 1, rows, cols] = low
        if t >= 2 and CHI > 1:
            row = lax.broadcasted_iota(jnp.int32, (CB, CB), 0)
            lane = lax.broadcasted_iota(jnp.int32, (CB, CB), 1)
            if t == 2:
                c, lo, h = lane // (CLO * T), (lane // T) % CLO, lane % T
            else:
                lo, c, h = lane // (CHI * T), (lane // T) % CHI, lane % T
            move = (row == (lo * T + h) * CHI + c).astype(jnp.float32).astype(jnp.bfloat16)
            for v in range(2):
                for i in range(2):
                    for p in range(2):
                        cols = slice(p * CB, (p + 1) * CB)
                        w[v, i, :, cols] = jnp.dot(
                            w[v, i, :, cols], move, preferred_element_type=jnp.float32
                        ).astype(jnp.bfloat16)

    def merge(t, v, real, imag):
        rh, rl = split(real)
        ih, il = split(imag)
        ah = jnp.concatenate([jnp.concatenate([rh, -ih], axis=1), jnp.concatenate([ih, rh], axis=1)], axis=0)
        al = jnp.concatenate([jnp.concatenate([rl, -il], axis=1), jnp.concatenate([il, rl], axis=1)], axis=0)
        dims = (((1,), (1,)), ((), ()))
        dot = functools.partial(lax.dot_general, dimension_numbers=dims,
                                preferred_element_type=jnp.float32)
        wh, wl = ws[t][v, 0], ws[t][v, 1]
        return dot(wh, ah) + (dot(wh, al) + dot(wl, ah))

    def regroup(ref, chi_major):
        rows = CB // CLO
        pieces = []
        for lo in range(CLO):
            if chi_major:
                pieces.append(jnp.concatenate(
                    [ref[pl.ds(c * CLO + lo, T, stride=K), :] for c in range(CHI)], axis=0))
            else:
                pieces.append(ref[pl.ds(lo, rows, stride=CLO), :])
        return [jnp.concatenate([b[:, p * M:(p + 1) * M] for b in pieces], axis=1) for p in range(2)]

    for t in range(4):
        launch(t)
    lead(0)
    pending = [(first, 0), (first, 1), (second, 0), (second, 1), (third, 0), (first, 2), (third, 1),
               (first, 3), (second, 2), (second, 3), (third, 2), (third, 3)]

    def more(count):
        for _ in range(min(count, len(pending))):
            action, t = pending.pop(0)
            action(t)

    more(5)
    for t in range(4):
        gs[t][0, 0, 0] = shard[t]
    load_tables(0)
    for s in range(S):
        y[s] = merge(0, values[s, 0], stem[s, 0], stem[s, 1])
        if s % 2:
            more(1)
    load_tables(1)
    rows_of = lambda s, i: pl.ds(pl.multiple_of((s * T + i) * K, K), K)
    for s in range(S):
        real, imag = regroup(y.at[s], True)
        sent[pl.ds(s * T * K, T * K), :] = merge(1, values[s, 1], real, imag)
        for d in range(1, T):
            to = lax.rem(me + d, T)
            push(sent.at[rows_of(s, to)], got.at[rows_of(s, me)], xs_sem.at[s, d], x_sem.at[s, d], (gx, to))
        got[rows_of(s, me), :] = sent[rows_of(s, me), :]
        more(1)
    more(len(pending))
    load_tables(2)
    load_tables(3)
    sums = [None, None]
    for s in range(S):
        for d in range(1, T):
            frm = lax.rem(me - d + T, T)
            arrived(got.at[rows_of(s, frm)], x_sem.at[s, d])
        parts = [[], []]
        for hi in range(CHI):
            block = jnp.concatenate(
                [got[pl.ds(s * T * K + hi * CLO + lo, T, stride=K), :] for lo in range(CLO)], axis=0)
            turned = block.T
            for p in range(2):
                parts[p].append(jnp.concatenate(
                    [turned[(p * CHI + c) * T:(p * CHI + c + 1) * T] for c in range(CHI)], axis=1))
        real, imag = [jnp.concatenate(q, axis=0) for q in parts]
        r = merge(2, values[s, 2], real, imag)
        one = values[s, 3] == 1
        for v in range(2):
            part = jnp.where(one if v else jnp.logical_not(one), r, 0.0)
            sums[v] = part if s == 0 else sums[v] + part
    y[0] = sums[0]
    y[1] = sums[1]
    total = None
    for v in range(2):
        real, imag = regroup(y.at[v], False)
        r = merge(3, v, real, imag)
        total = r if v == 0 else total + r
    fsent[...] = total
    row_of = lambda i: pl.ds(pl.multiple_of(i * K, K), K)
    for d in range(1, T):
        to = lax.rem(me + d, T)
        push(fsent.at[row_of(to)], fgot.at[row_of(me)], fs_sem.at[d], f_sem.at[d], (gx, to))
    fgot[row_of(me), :] = fsent[row_of(me), :]
    for d in range(1, T):
        frm = lax.rem(me - d + T, T)
        arrived(fgot.at[row_of(frm)], f_sem.at[d])

    lanes = 2 * M
    width = lanes // CHI
    across = jnp.concatenate([fgot[pl.ds(c, T, stride=K), :] for c in range(K)], axis=0)
    halves = CB // lanes
    for i in range(halves):
        turned_f[i] = across[i * lanes:(i + 1) * lanes].T
    pieces = [jnp.concatenate(
        [turned_f[i, pl.ds(c, 2 * T, stride=CHI), :] for i in range(halves)], axis=1) for c in range(CHI)]
    count = CB // width
    lined = jnp.concatenate(
        [jnp.concatenate([q[:, j * width:(j + 1) * width] for q in pieces], axis=1) for j in range(count)], axis=0)
    row = lax.broadcasted_iota(jnp.int32, (lanes, lanes), 0)
    lane = lax.broadcasted_iota(jnp.int32, (lanes, lanes), 1)
    move = (row == (lane % CHI) * width + lane // CHI).astype(jnp.float32).astype(jnp.bfloat16)
    first, rest = lined.astype(jnp.bfloat16), lined
    rest = rest - first.astype(jnp.float32)
    second, third = split(rest)
    dot = functools.partial(jnp.dot, preferred_element_type=jnp.float32)
    placed = (dot(first, move) + dot(second, move)) + dot(third, move)
    for j in range(count):
        out[:, j * lanes:(j + 1) * lanes] = placed[j * 2 * T:(j + 1) * 2 * T]
    for copy in started:
        copy.wait_send()


def fused_device(stem_field, branches, branch_order, slice_values):
    T = lax.axis_size("tensor")
    S, _, entries = stem_field.shape
    steps, _, _, CB, K = branches.shape
    M = entries // CB
    CLO = CB // M
    CHI = K // CLO
    stem = stem_field.reshape(S, 2, M, CB)
    shard = jnp.take(branches, branch_order, axis=0).reshape(steps, 4, CB, K).transpose(0, 1, 3, 2)
    vmem = pl.BlockSpec(memory_space=pltpu.VMEM)
    dma = pltpu.SemaphoreType.DMA
    table = pltpu.VMEM((2, 2, T // 4, 4, K, CB), jnp.float32)
    merged = pltpu.VMEM((2, 2, CB, 2 * CB), jnp.bfloat16)
    moved = pltpu.VMEM((T * S * K, 2 * M), jnp.float32)
    gathered = pl.pallas_call(
        functools.partial(kernel, (T, S, K, CB, M, CLO, CHI)),
        out_shape=jax.ShapeDtypeStruct((2 * T, entries // T), jnp.float32),
        in_specs=[pl.BlockSpec(memory_space=pltpu.SMEM), vmem, vmem],
        out_specs=vmem,
        scratch_shapes=[
            table, table, table, table,
            merged, merged, merged, merged,
            pltpu.VMEM((S, CB, 2 * M), jnp.float32),
            moved, moved,
            pltpu.VMEM((CB, 2 * M), jnp.float32),
            pltpu.VMEM((CB, 2 * M), jnp.float32),
            pltpu.VMEM((CB // (2 * M), 2 * M, 2 * M), jnp.float32),
            dma((4, 11 + T // 4)), dma((4, 11 + T // 4)),
            dma((S, T)), dma((T,)), dma((S, T)), dma((T,)),
        ],
        compiler_params=pltpu.CompilerParams(collective_id=0, has_side_effects=True),
    )(slice_values, stem, shard)
    return gathered.reshape(2, entries)


def solution(mesh):
    def per_device(stem_field, branches, branch_order, slice_values):
        shards = lax.axis_size("tensor")
        steps, _, _, width, columns = branches.shape
        middle = stem_field.shape[2] // width
        fits = (
            mesh.shape["groups"] == 2 and shards % 8 == 0 and columns % 8 == 0 and steps == 4
            and 2 * middle == 128 and width % middle == 0 and columns % (width // middle) == 0
        )
        run = fused_device if fits else plain_device
        return run(stem_field, branches, branch_order, slice_values)

    return jax.shard_map(
        per_device,
        mesh=mesh,
        in_specs=(
            P("groups", None, "tensor"),
            P(None, None, None, None, "tensor"),
            P(),
            P("groups", None),
        ),
        out_specs=P("groups", "tensor"),
        check_vma=False,
    )
```

```python
import functools

import jax
import jax.numpy as jnp
from jax import lax
from jax.experimental import pallas as pl
from jax.experimental.pallas import tpu as pltpu
from jax.sharding import PartitionSpec as P

MESH = pl.DeviceIdType.MESH


def product(left, right):
    return jnp.einsum("smi,sil->slm", left, right, precision=lax.Precision.HIGHEST)


def combine_branch(stem_part, branch_now, values_now):
    slices, _, _, width = stem_part.shape
    chosen = jnp.where(
        (values_now == 1)[:, None, None, None], branch_now[1][None], branch_now[0][None]
    )
    real_part = product(stem_part[:, 0], chosen[:, 0]) - product(stem_part[:, 1], chosen[:, 1])
    imag_part = product(stem_part[:, 0], chosen[:, 1]) + product(stem_part[:, 1], chosen[:, 0])
    return jnp.stack([real_part, imag_part], axis=1)


def plain_device(stem_field, branches, branch_order, slice_values):
    shards = lax.axis_size("tensor")
    steps = branches.shape[0]
    width = branches.shape[3]
    current = stem_field
    for step in range(steps):
        table = lax.all_gather(
            lax.dynamic_index_in_dim(branches, branch_order[step], 0, keepdims=False),
            "tensor",
            axis=3,
            tiled=True,
        )
        slices, parts, entries = current.shape
        blocks = current.reshape(slices, parts, entries // width, width)
        combined = combine_branch(blocks, table, slice_values[:, step])
        combined = combined.reshape(slices, parts, shards, width // shards, entries // width)
        current = lax.all_to_all(
            combined, "tensor", split_axis=2, concat_axis=2, tiled=True
        ).reshape(current.shape)
    return jnp.sum(current, axis=0)


def split(value):
    high = value.astype(jnp.bfloat16)
    return high, (value - high.astype(jnp.float32)).astype(jnp.bfloat16)


def kernel(cfg, values, stem, shard, out, g0, g1, g2, g3, w0, w1, w2, w3, y, sent, got, fsent, fgot, turned_f,
           gather_sem, send_sem, x_sem, f_sem, xs_sem, fs_sem):
    T, S, K, CB, M, CLO, CHI = cfg
    Z = T // 4
    gs = (g0, g1, g2, g3)
    ws = (w0, w1, w2, w3)
    gx = lax.axis_index("groups")
    me = lax.axis_index("tensor")
    core = lax.rem(me, 2)
    col = lax.rem(me // 2, 2)
    depth = me // 4
    partner = me + 1 - 2 * core
    across_y = me + 2 - 4 * col

    barrier = pltpu.get_barrier_semaphore()
    for d in range(1, T):
        pl.semaphore_signal(barrier, inc=1, device_id=(gx, lax.rem(me + d, T)), device_id_type=MESH)
    pl.semaphore_signal(barrier, inc=1, device_id=(1 - gx, me), device_id_type=MESH)
    pl.semaphore_wait(barrier, T)

    started = []
    counter = [0] * 4
    ours = pl.ds(2 * gx, 2)
    theirs = pl.ds(2 - 2 * gx, 2)
    far = pl.ds(1, Z - 1)

    def push(src, dst, ssem, rsem, device):
        copy = pltpu.make_async_remote_copy(
            src_ref=src, dst_ref=dst, send_sem=ssem, recv_sem=rsem,
            device_id=device, device_id_type=MESH,
        )
        copy.start()
        started.append(copy)

    def arrived(dst, rsem):
        pltpu.make_async_remote_copy(
            src_ref=dst, dst_ref=dst, send_sem=rsem, recv_sem=rsem,
            device_id=(gx, partner), device_id_type=MESH).wait_recv()

    def token(t):
        counter[t] += 1
        return send_sem.at[t, counter[t] - 1]

    def send(t, src, dst, slot, device):
        push(src, dst, token(t), gather_sem.at[t, slot], device)

    def pair(t, row, levels, part, slot):
        send(t, gs[t].at[0, row, levels, part], gs[t].at[1, row, levels, part], slot, (gx, partner))

    def side(t, row, slot):
        src = gs[t].at[0, row, far, ours]
        send(t, src, src, slot, (1 - gx, me))

    def launch(t):
        for d in range(1, Z):
            to = lax.rem(depth + d, Z) * 4 + lax.rem(me, 4)
            send(t, shard.at[t, ours], gs[t].at[0, 0, Z - d, ours], 11 + Z - d, (gx, to))

    def lead(t):
        send(t, shard.at[t], gs[t].at[0, 1, 0], 0, (gx, across_y))
        send(t, shard.at[t], gs[t].at[1, 0, 0], 5, (gx, partner))

    def first(t):
        for d in range(1, Z):
            arrived(gs[t].at[0, 0, d, ours], gather_sem.at[t, 11 + d])
        send(t, gs[t].at[0, 0, far, ours], gs[t].at[0, 1, far, ours], 1, (gx, across_y))
        side(t, 0, 2)
        pair(t, 0, far, ours, 6)
        if t < 2:
            lead(t + 2)

    def second(t):
        arrived(gs[t].at[0, 1, far, ours], gather_sem.at[t, 1])
        side(t, 1, 3)
        pair(t, 1, far, ours, 7)
        arrived(gs[t].at[0, 1, 0], gather_sem.at[t, 0])
        send(t, gs[t].at[0, 1, 0], gs[t].at[1, 1, 0], 8, (gx, partner))

    def third(t):
        arrived(gs[t].at[0, 0, far, theirs], gather_sem.at[t, 2])
        pair(t, 0, far, theirs, 9)
        arrived(gs[t].at[0, 1, far, theirs], gather_sem.at[t, 3])
        pair(t, 1, far, theirs, 10)

    def settle(t):
        arrived(gs[t].at[1, 0, 0], gather_sem.at[t, 5])
        arrived(gs[t].at[1, 0, far, ours], gather_sem.at[t, 6])
        arrived(gs[t].at[1, 1, far, ours], gather_sem.at[t, 7])
        arrived(gs[t].at[1, 1, 0], gather_sem.at[t, 8])
        arrived(gs[t].at[1, 0, far, theirs], gather_sem.at[t, 9])
        arrived(gs[t].at[1, 1, far, theirs], gather_sem.at[t, 10])

    def load_tables(t):
        settle(t)
        g, w = gs[t], ws[t]
        for a in range(T):
            z, c, which = a // 4, (a // 2) % 2, a % 2
            rel = lax.rem(z - depth + Z, Z)
            row = jnp.where(col == c, 0, 1)
            other = jnp.where(core == which, 0, 1)
            for v in range(2):
                for p in range(2):
                    high, low = split(g[other, row, rel, 2 * v + p])
                    rows = slice(a * K, (a + 1) * K)
                    cols = slice(p * CB, (p + 1) * CB)
                    w[v, 0, rows, cols] = high
                    w[v, 1, rows, cols] = low
        if t >= 2 and CHI > 1:
            row = lax.broadcasted_iota(jnp.int32, (CB, CB), 0)
            lane = lax.broadcasted_iota(jnp.int32, (CB, CB), 1)
            if t == 2:
                c, lo, h = lane // (CLO * T), (lane // T) % CLO, lane % T
            else:
                lo, c, h = lane // (CHI * T), (lane // T) % CHI, lane % T
            move = (row == (lo * T + h) * CHI + c).astype(jnp.float32).astype(jnp.bfloat16)
            for v in range(2):
                for i in range(2):
                    for p in range(2):
                        cols = slice(p * CB, (p + 1) * CB)
                        w[v, i, :, cols] = jnp.dot(
                            w[v, i, :, cols], move, preferred_element_type=jnp.float32
                        ).astype(jnp.bfloat16)

    def merge(t, v, real, imag):
        rh, rl = split(real)
        ih, il = split(imag)
        ah = jnp.concatenate([jnp.concatenate([rh, -ih], axis=1), jnp.concatenate([ih, rh], axis=1)], axis=0)
        al = jnp.concatenate([jnp.concatenate([rl, -il], axis=1), jnp.concatenate([il, rl], axis=1)], axis=0)
        dims = (((1,), (1,)), ((), ()))
        dot = functools.partial(lax.dot_general, dimension_numbers=dims,
                                preferred_element_type=jnp.float32)
        wh, wl = ws[t][v, 0], ws[t][v, 1]
        return dot(wh, ah) + (dot(wh, al) + dot(wl, ah))

    def regroup(ref, chi_major):
        rows = CB // CLO
        pieces = []
        for lo in range(CLO):
            if chi_major:
                pieces.append(jnp.concatenate(
                    [ref[pl.ds(c * CLO + lo, T, stride=K), :] for c in range(CHI)], axis=0))
            else:
                pieces.append(ref[pl.ds(lo, rows, stride=CLO), :])
        return [jnp.concatenate([b[:, p * M:(p + 1) * M] for b in pieces], axis=1) for p in range(2)]

    for t in range(4):
        launch(t)
    lead(0)
    lead(1)
    pending = [(first, 0), (first, 1), (second, 0), (second, 1), (third, 0), (first, 2), (third, 1),
               (first, 3), (second, 2), (second, 3), (third, 2), (third, 3)]

    def more(count):
        for _ in range(min(count, len(pending))):
            action, t = pending.pop(0)
            action(t)

    more(5)
    for t in range(4):
        gs[t][0, 0, 0] = shard[t]
    load_tables(0)
    for s in range(S):
        y[s] = merge(0, values[s, 0], stem[s, 0], stem[s, 1])
        if s % 2:
            more(1)
    load_tables(1)
    rows_of = lambda s, i: pl.ds(pl.multiple_of((s * T + i) * K, K), K)
    for s in range(S):
        real, imag = regroup(y.at[s], True)
        sent[pl.ds(s * T * K, T * K), :] = merge(1, values[s, 1], real, imag)
        for d in range(1, T):
            to = lax.rem(me + d, T)
            push(sent.at[rows_of(s, to)], got.at[rows_of(s, me)], xs_sem.at[s, d], x_sem.at[s, d], (gx, to))
        got[rows_of(s, me), :] = sent[rows_of(s, me), :]
        more(1)
    more(len(pending))
    load_tables(2)
    load_tables(3)
    sums = [None, None]
    for s in range(S):
        for d in range(1, T):
            frm = lax.rem(me - d + T, T)
            arrived(got.at[rows_of(s, frm)], x_sem.at[s, d])
        parts = [[], []]
        for hi in range(CHI):
            block = jnp.concatenate(
                [got[pl.ds(s * T * K + hi * CLO + lo, T, stride=K), :] for lo in range(CLO)], axis=0)
            turned = block.T
            for p in range(2):
                parts[p].append(jnp.concatenate(
                    [turned[(p * CHI + c) * T:(p * CHI + c + 1) * T] for c in range(CHI)], axis=1))
        real, imag = [jnp.concatenate(q, axis=0) for q in parts]
        r = merge(2, values[s, 2], real, imag)
        one = values[s, 3] == 1
        for v in range(2):
            part = jnp.where(one if v else jnp.logical_not(one), r, 0.0)
            sums[v] = part if s == 0 else sums[v] + part
    y[0] = sums[0]
    y[1] = sums[1]
    total = None
    for v in range(2):
        real, imag = regroup(y.at[v], False)
        r = merge(3, v, real, imag)
        total = r if v == 0 else total + r
    fsent[...] = total
    row_of = lambda i: pl.ds(pl.multiple_of(i * K, K), K)
    for d in range(1, T):
        to = lax.rem(me + d, T)
        push(fsent.at[row_of(to)], fgot.at[row_of(me)], fs_sem.at[d], f_sem.at[d], (gx, to))
    fgot[row_of(me), :] = fsent[row_of(me), :]
    for d in range(1, T):
        frm = lax.rem(me - d + T, T)
        arrived(fgot.at[row_of(frm)], f_sem.at[d])

    lanes = 2 * M
    width = lanes // CHI
    across = jnp.concatenate([fgot[pl.ds(c, T, stride=K), :] for c in range(K)], axis=0)
    halves = CB // lanes
    for i in range(halves):
        turned_f[i] = across[i * lanes:(i + 1) * lanes].T
    pieces = [jnp.concatenate(
        [turned_f[i, pl.ds(c, 2 * T, stride=CHI), :] for i in range(halves)], axis=1) for c in range(CHI)]
    count = CB // width
    lined = jnp.concatenate(
        [jnp.concatenate([q[:, j * width:(j + 1) * width] for q in pieces], axis=1) for j in range(count)], axis=0)
    row = lax.broadcasted_iota(jnp.int32, (lanes, lanes), 0)
    lane = lax.broadcasted_iota(jnp.int32, (lanes, lanes), 1)
    move = (row == (lane % CHI) * width + lane // CHI).astype(jnp.float32).astype(jnp.bfloat16)
    first, rest = lined.astype(jnp.bfloat16), lined
    rest = rest - first.astype(jnp.float32)
    second, third = split(rest)
    dot = functools.partial(jnp.dot, preferred_element_type=jnp.float32)
    placed = (dot(first, move) + dot(second, move)) + dot(third, move)
    for j in range(count):
        out[:, j * lanes:(j + 1) * lanes] = placed[j * 2 * T:(j + 1) * 2 * T]
    for copy in started:
        copy.wait_send()


def fused_device(stem_field, branches, branch_order, slice_values):
    T = lax.axis_size("tensor")
    S, _, entries = stem_field.shape
    steps, _, _, CB, K = branches.shape
    M = entries // CB
    CLO = CB // M
    CHI = K // CLO
    stem = stem_field.reshape(S, 2, M, CB)
    shard = branches.at[branch_order].get(mode="promise_in_bounds").reshape(steps, 4, CB, K).transpose(0, 1, 3, 2)
    vmem = pl.BlockSpec(memory_space=pltpu.VMEM)
    dma = pltpu.SemaphoreType.DMA
    table = pltpu.VMEM((2, 2, T // 4, 4, K, CB), jnp.float32)
    merged = pltpu.VMEM((2, 2, CB, 2 * CB), jnp.bfloat16)
    moved = pltpu.VMEM((T * S * K, 2 * M), jnp.float32)
    gathered = pl.pallas_call(
        functools.partial(kernel, (T, S, K, CB, M, CLO, CHI)),
        out_shape=jax.ShapeDtypeStruct((2 * T, entries // T), jnp.float32),
        in_specs=[pl.BlockSpec(memory_space=pltpu.SMEM), vmem, vmem],
        out_specs=vmem,
        scratch_shapes=[
            table, table, table, table,
            merged, merged, merged, merged,
            pltpu.VMEM((S, CB, 2 * M), jnp.float32),
            moved, moved,
            pltpu.VMEM((CB, 2 * M), jnp.float32),
            pltpu.VMEM((CB, 2 * M), jnp.float32),
            pltpu.VMEM((CB // (2 * M), 2 * M, 2 * M), jnp.float32),
            dma((4, 11 + T // 4)), dma((4, 11 + T // 4)),
            dma((S, T)), dma((T,)), dma((S, T)), dma((T,)),
        ],
        compiler_params=pltpu.CompilerParams(collective_id=0, has_side_effects=True),
    )(slice_values, stem, shard)
    return gathered.reshape(2, entries)


def solution(mesh):
    def per_device(stem_field, branches, branch_order, slice_values):
        shards = lax.axis_size("tensor")
        steps, _, _, width, columns = branches.shape
        middle = stem_field.shape[2] // width
        fits = (
            mesh.shape["groups"] == 2 and shards % 8 == 0 and columns % 8 == 0 and steps == 4
            and 2 * middle == 128 and width % middle == 0 and columns % (width // middle) == 0
        )
        run = fused_device if fits else plain_device
        return run(stem_field, branches, branch_order, slice_values)

    return jax.shard_map(
        per_device,
        mesh=mesh,
        in_specs=(
            P("groups", None, "tensor"),
            P(None, None, None, None, "tensor"),
            P(),
            P("groups", None),
        ),
        out_specs=P("groups", "tensor"),
        check_vma=False,
    )
```

```python
import functools

import jax
import jax.numpy as jnp
from jax import lax
from jax.experimental import pallas as pl
from jax.experimental.pallas import tpu as pltpu
from jax.sharding import PartitionSpec as P

MESH = pl.DeviceIdType.MESH


def product(left, right):
    return jnp.einsum("smi,sil->slm", left, right, precision=lax.Precision.HIGHEST)


def combine_branch(stem_part, branch_now, values_now):
    slices, _, _, width = stem_part.shape
    chosen = jnp.where(
        (values_now == 1)[:, None, None, None], branch_now[1][None], branch_now[0][None]
    )
    real_part = product(stem_part[:, 0], chosen[:, 0]) - product(stem_part[:, 1], chosen[:, 1])
    imag_part = product(stem_part[:, 0], chosen[:, 1]) + product(stem_part[:, 1], chosen[:, 0])
    return jnp.stack([real_part, imag_part], axis=1)


def plain_device(stem_field, branches, branch_order, slice_values):
    shards = lax.axis_size("tensor")
    steps = branches.shape[0]
    width = branches.shape[3]
    current = stem_field
    for step in range(steps):
        table = lax.all_gather(
            lax.dynamic_index_in_dim(branches, branch_order[step], 0, keepdims=False),
            "tensor",
            axis=3,
            tiled=True,
        )
        slices, parts, entries = current.shape
        blocks = current.reshape(slices, parts, entries // width, width)
        combined = combine_branch(blocks, table, slice_values[:, step])
        combined = combined.reshape(slices, parts, shards, width // shards, entries // width)
        current = lax.all_to_all(
            combined, "tensor", split_axis=2, concat_axis=2, tiled=True
        ).reshape(current.shape)
    return jnp.sum(current, axis=0)


def split(value):
    high = value.astype(jnp.bfloat16)
    return high, (value - high.astype(jnp.float32)).astype(jnp.bfloat16)


def kernel(cfg, values, stem, shard, out, g0, g1, g2, g3, w0, w1, w2, w3, y, sent, got, fsent, fgot, turned_f,
           gather_sem, send_sem, x_sem, f_sem, xs_sem, fs_sem):
    T, S, K, CB, M, CLO, CHI = cfg
    Z = T // 4
    gs = (g0, g1, g2, g3)
    ws = (w0, w1, w2, w3)
    gx = lax.axis_index("groups")
    me = lax.axis_index("tensor")
    core = lax.rem(me, 2)
    col = lax.rem(me // 2, 2)
    depth = me // 4
    partner = me + 1 - 2 * core
    across_y = me + 2 - 4 * col

    barrier = pltpu.get_barrier_semaphore()
    for d in range(1, T):
        pl.semaphore_signal(barrier, inc=1, device_id=(gx, lax.rem(me + d, T)), device_id_type=MESH)
    pl.semaphore_signal(barrier, inc=1, device_id=(1 - gx, me), device_id_type=MESH)
    pl.semaphore_wait(barrier, T)

    started = []
    counter = [0] * 4
    ours = pl.ds(2 * gx, 2)
    theirs = pl.ds(2 - 2 * gx, 2)
    far = pl.ds(1, Z - 1)

    def push(src, dst, ssem, rsem, device):
        copy = pltpu.make_async_remote_copy(
            src_ref=src, dst_ref=dst, send_sem=ssem, recv_sem=rsem,
            device_id=device, device_id_type=MESH,
        )
        copy.start()
        started.append(copy)

    def arrived(dst, rsem):
        pltpu.make_async_remote_copy(
            src_ref=dst, dst_ref=dst, send_sem=rsem, recv_sem=rsem,
            device_id=(gx, partner), device_id_type=MESH).wait_recv()

    def token(t):
        counter[t] += 1
        return send_sem.at[t, counter[t] - 1]

    def send(t, src, dst, slot, device):
        push(src, dst, token(t), gather_sem.at[t, slot], device)

    def pair(t, row, levels, part, slot):
        send(t, gs[t].at[0, row, levels, part], gs[t].at[1, row, levels, part], slot, (gx, partner))

    def side(t, row, slot):
        src = gs[t].at[0, row, far, ours]
        send(t, src, src, slot, (1 - gx, me))

    def launch(t):
        for d in range(1, Z):
            to = lax.rem(depth + d, Z) * 4 + lax.rem(me, 4)
            send(t, shard.at[t, ours], gs[t].at[0, 0, Z - d, ours], 11 + Z - d, (gx, to))

    def lead(t):
        send(t, shard.at[t], gs[t].at[0, 1, 0], 0, (gx, across_y))
        send(t, shard.at[t], gs[t].at[1, 0, 0], 5, (gx, partner))

    def first(t):
        for d in range(1, Z):
            arrived(gs[t].at[0, 0, d, ours], gather_sem.at[t, 11 + d])
        send(t, gs[t].at[0, 0, far, ours], gs[t].at[0, 1, far, ours], 1, (gx, across_y))
        side(t, 0, 2)
        pair(t, 0, far, ours, 6)
        if t < 2:
            launch(t + 2)
            lead(t + 2)

    def second(t):
        arrived(gs[t].at[0, 1, far, ours], gather_sem.at[t, 1])
        side(t, 1, 3)
        pair(t, 1, far, ours, 7)
        arrived(gs[t].at[0, 1, 0], gather_sem.at[t, 0])
        send(t, gs[t].at[0, 1, 0], gs[t].at[1, 1, 0], 8, (gx, partner))

    def third(t):
        arrived(gs[t].at[0, 0, far, theirs], gather_sem.at[t, 2])
        pair(t, 0, far, theirs, 9)
        arrived(gs[t].at[0, 1, far, theirs], gather_sem.at[t, 3])
        pair(t, 1, far, theirs, 10)

    def settle(t):
        arrived(gs[t].at[1, 0, 0], gather_sem.at[t, 5])
        arrived(gs[t].at[1, 0, far, ours], gather_sem.at[t, 6])
        arrived(gs[t].at[1, 1, far, ours], gather_sem.at[t, 7])
        arrived(gs[t].at[1, 1, 0], gather_sem.at[t, 8])
        arrived(gs[t].at[1, 0, far, theirs], gather_sem.at[t, 9])
        arrived(gs[t].at[1, 1, far, theirs], gather_sem.at[t, 10])

    def load_tables(t):
        settle(t)
        g, w = gs[t], ws[t]
        for a in range(T):
            z, c, which = a // 4, (a // 2) % 2, a % 2
            rel = lax.rem(z - depth + Z, Z)
            row = jnp.where(col == c, 0, 1)
            other = jnp.where(core == which, 0, 1)
            for v in range(2):
                for p in range(2):
                    high, low = split(g[other, row, rel, 2 * v + p])
                    rows = slice(a * K, (a + 1) * K)
                    cols = slice(p * CB, (p + 1) * CB)
                    w[v, 0, rows, cols] = high
                    w[v, 1, rows, cols] = low
        if t >= 2 and CHI > 1:
            row = lax.broadcasted_iota(jnp.int32, (CB, CB), 0)
            lane = lax.broadcasted_iota(jnp.int32, (CB, CB), 1)
            if t == 2:
                c, lo, h = lane // (CLO * T), (lane // T) % CLO, lane % T
            else:
                lo, c, h = lane // (CHI * T), (lane // T) % CHI, lane % T
            move = (row == (lo * T + h) * CHI + c).astype(jnp.float32).astype(jnp.bfloat16)
            for v in range(2):
                for i in range(2):
                    for p in range(2):
                        cols = slice(p * CB, (p + 1) * CB)
                        w[v, i, :, cols] = jnp.dot(
                            w[v, i, :, cols], move, preferred_element_type=jnp.float32
                        ).astype(jnp.bfloat16)

    def merge(t, v, real, imag):
        rh, rl = split(real)
        ih, il = split(imag)
        ah = jnp.concatenate([jnp.concatenate([rh, -ih], axis=1), jnp.concatenate([ih, rh], axis=1)], axis=0)
        al = jnp.concatenate([jnp.concatenate([rl, -il], axis=1), jnp.concatenate([il, rl], axis=1)], axis=0)
        dims = (((1,), (1,)), ((), ()))
        dot = functools.partial(lax.dot_general, dimension_numbers=dims,
                                preferred_element_type=jnp.float32)
        wh, wl = ws[t][v, 0], ws[t][v, 1]
        return dot(wh, ah) + (dot(wh, al) + dot(wl, ah))

    def regroup(ref, chi_major):
        rows = CB // CLO
        pieces = []
        for lo in range(CLO):
            if chi_major:
                pieces.append(jnp.concatenate(
                    [ref[pl.ds(c * CLO + lo, T, stride=K), :] for c in range(CHI)], axis=0))
            else:
                pieces.append(ref[pl.ds(lo, rows, stride=CLO), :])
        return [jnp.concatenate([b[:, p * M:(p + 1) * M] for b in pieces], axis=1) for p in range(2)]

    for t in range(2):
        launch(t)
    lead(0)
    lead(1)
    pending = [(first, 0), (first, 1), (second, 0), (second, 1), (third, 0), (first, 2), (third, 1),
               (first, 3), (second, 2), (second, 3), (third, 2), (third, 3)]

    def more(count):
        for _ in range(min(count, len(pending))):
            action, t = pending.pop(0)
            action(t)

    more(5)
    for t in range(4):
        gs[t][0, 0, 0] = shard[t]
    load_tables(0)
    for s in range(S):
        y[s] = merge(0, values[s, 0], stem[s, 0], stem[s, 1])
        if s % 2:
            more(1)
    load_tables(1)
    rows_of = lambda s, i: pl.ds(pl.multiple_of((s * T + i) * K, K), K)
    for s in range(S):
        real, imag = regroup(y.at[s], True)
        sent[pl.ds(s * T * K, T * K), :] = merge(1, values[s, 1], real, imag)
        for d in range(1, T):
            to = lax.rem(me + d, T)
            push(sent.at[rows_of(s, to)], got.at[rows_of(s, me)], xs_sem.at[s, d], x_sem.at[s, d], (gx, to))
        got[rows_of(s, me), :] = sent[rows_of(s, me), :]
        more(1)
    more(len(pending))
    load_tables(2)
    load_tables(3)
    sums = [None, None]
    for s in range(S):
        for d in range(1, T):
            frm = lax.rem(me - d + T, T)
            arrived(got.at[rows_of(s, frm)], x_sem.at[s, d])
        parts = [[], []]
        for hi in range(CHI):
            block = jnp.concatenate(
                [got[pl.ds(s * T * K + hi * CLO + lo, T, stride=K), :] for lo in range(CLO)], axis=0)
            turned = block.T
            for p in range(2):
                parts[p].append(jnp.concatenate(
                    [turned[(p * CHI + c) * T:(p * CHI + c + 1) * T] for c in range(CHI)], axis=1))
        real, imag = [jnp.concatenate(q, axis=0) for q in parts]
        r = merge(2, values[s, 2], real, imag)
        one = values[s, 3] == 1
        for v in range(2):
            part = jnp.where(one if v else jnp.logical_not(one), r, 0.0)
            sums[v] = part if s == 0 else sums[v] + part
    y[0] = sums[0]
    y[1] = sums[1]
    total = None
    for v in range(2):
        real, imag = regroup(y.at[v], False)
        r = merge(3, v, real, imag)
        total = r if v == 0 else total + r
    fsent[...] = total
    row_of = lambda i: pl.ds(pl.multiple_of(i * K, K), K)
    for d in range(1, T):
        to = lax.rem(me + d, T)
        push(fsent.at[row_of(to)], fgot.at[row_of(me)], fs_sem.at[d], f_sem.at[d], (gx, to))
    fgot[row_of(me), :] = fsent[row_of(me), :]
    for d in range(1, T):
        frm = lax.rem(me - d + T, T)
        arrived(fgot.at[row_of(frm)], f_sem.at[d])

    lanes = 2 * M
    width = lanes // CHI
    across = jnp.concatenate([fgot[pl.ds(c, T, stride=K), :] for c in range(K)], axis=0)
    halves = CB // lanes
    for i in range(halves):
        turned_f[i] = across[i * lanes:(i + 1) * lanes].T
    pieces = [jnp.concatenate(
        [turned_f[i, pl.ds(c, 2 * T, stride=CHI), :] for i in range(halves)], axis=1) for c in range(CHI)]
    count = CB // width
    lined = jnp.concatenate(
        [jnp.concatenate([q[:, j * width:(j + 1) * width] for q in pieces], axis=1) for j in range(count)], axis=0)
    row = lax.broadcasted_iota(jnp.int32, (lanes, lanes), 0)
    lane = lax.broadcasted_iota(jnp.int32, (lanes, lanes), 1)
    move = (row == (lane % CHI) * width + lane // CHI).astype(jnp.float32).astype(jnp.bfloat16)
    first, rest = lined.astype(jnp.bfloat16), lined
    rest = rest - first.astype(jnp.float32)
    second, third = split(rest)
    dot = functools.partial(jnp.dot, preferred_element_type=jnp.float32)
    placed = (dot(first, move) + dot(second, move)) + dot(third, move)
    for j in range(count):
        out[:, j * lanes:(j + 1) * lanes] = placed[j * 2 * T:(j + 1) * 2 * T]
    for copy in started:
        copy.wait_send()


def fused_device(stem_field, branches, branch_order, slice_values):
    T = lax.axis_size("tensor")
    S, _, entries = stem_field.shape
    steps, _, _, CB, K = branches.shape
    M = entries // CB
    CLO = CB // M
    CHI = K // CLO
    stem = stem_field.reshape(S, 2, M, CB)
    shard = branches.at[branch_order].get(mode="promise_in_bounds").reshape(steps, 4, CB, K).transpose(0, 1, 3, 2)
    vmem = pl.BlockSpec(memory_space=pltpu.VMEM)
    dma = pltpu.SemaphoreType.DMA
    table = pltpu.VMEM((2, 2, T // 4, 4, K, CB), jnp.float32)
    merged = pltpu.VMEM((2, 2, CB, 2 * CB), jnp.bfloat16)
    moved = pltpu.VMEM((T * S * K, 2 * M), jnp.float32)
    gathered = pl.pallas_call(
        functools.partial(kernel, (T, S, K, CB, M, CLO, CHI)),
        out_shape=jax.ShapeDtypeStruct((2 * T, entries // T), jnp.float32),
        in_specs=[pl.BlockSpec(memory_space=pltpu.SMEM), vmem, vmem],
        out_specs=vmem,
        scratch_shapes=[
            table, table, table, table,
            merged, merged, merged, merged,
            pltpu.VMEM((S, CB, 2 * M), jnp.float32),
            moved, moved,
            pltpu.VMEM((CB, 2 * M), jnp.float32),
            pltpu.VMEM((CB, 2 * M), jnp.float32),
            pltpu.VMEM((CB // (2 * M), 2 * M, 2 * M), jnp.float32),
            dma((4, 11 + T // 4)), dma((4, 11 + T // 4)),
            dma((S, T)), dma((T,)), dma((S, T)), dma((T,)),
        ],
        compiler_params=pltpu.CompilerParams(collective_id=0, has_side_effects=True),
    )(slice_values, stem, shard)
    return gathered.reshape(2, entries)


def solution(mesh):
    def per_device(stem_field, branches, branch_order, slice_values):
        shards = lax.axis_size("tensor")
        steps, _, _, width, columns = branches.shape
        middle = stem_field.shape[2] // width
        fits = (
            mesh.shape["groups"] == 2 and shards % 8 == 0 and columns % 8 == 0 and steps == 4
            and 2 * middle == 128 and width % middle == 0 and columns % (width // middle) == 0
        )
        run = fused_device if fits else plain_device
        return run(stem_field, branches, branch_order, slice_values)

    return jax.shard_map(
        per_device,
        mesh=mesh,
        in_specs=(
            P("groups", None, "tensor"),
            P(None, None, None, None, "tensor"),
            P(),
            P("groups", None),
        ),
        out_specs=P("groups", "tensor"),
        check_vma=False,
    )
```
